32 devices in a mesh: replica: 4 (over y, z), dp: 8 (over x, core).
Axes of the slice: x: 4, y: 2, z: 2, core: 2. Of those that a mesh axis runs over, the one named last changes fastest.
The devices are a block of a 4x4x8 slice.
Arguments:
- x: bfloat16 [2048, 2048], P(('replica', 'dp')), parts along dimension 0
- lengths: int32 [2048], P(('replica', 'dp')), parts along dimension 0
- cache: bfloat16 [2, 2048, 128, 576], P(None, ('replica', 'dp')), parts along dimension 1
- attn_gain: float32 [2, 2048], replicated
- ffn_gain: float32 [2, 2048], replicated
- w_query: bfloat16 [2, 2048, 9216], replicated
- w_attn_out: bfloat16 [2, 8192, 2048], replicated
- w_up: bfloat16 [2, 2048, 11264], P(None, None, 'dp')
- w_gate: bfloat16 [2, 2048, 11264], P(None, None, 'dp')
- w_down: bfloat16 [2, 11264, 2048], P(None, 'dp')
Outputs:
- output: bfloat16 [2048, 2048], P(('replica', 'dp')), parts along dimension 0
There are 4 independent parts. The reference program is written for one: setup_inputs(seed, part) draws one part's arguments, and reference() takes and returns one part's arrays. A program takes and returns all parts, laid end to end along the dimension named above; an argument that names none is the same for every part.
All inputs are finite; a program needn't handle non-finite values.
Results may differ from the reference program's by a relative error of at most 0.02.
Values are sent between devices in bfloat16 or wider.
A program may use at most 768 MiB of HBM per device.

```python
import jax
import jax.numpy as jnp
from jax import lax

B_DEV = 64
GROUP_SIZE = 8
SEQ_LEN = 128
D_MODEL = 2048
FF_DIM = 11264
HEADS = 16
LATENT = 512
ROPE = 64
LAYERS = 2

NORM_EPS = 1e-6
BATCH = B_DEV * GROUP_SIZE
KV_DIM = LATENT + ROPE
SCORE_SCALE = (3 * ROPE) ** -0.5
LEN_FLOOR = max(1, SEQ_LEN // 16)
CAP_FLOOR = max(LEN_FLOOR, SEQ_LEN // 4)


def draw_lengths(key):
    cap_key, len_key, pick_key = jax.random.split(key, 3)
    caps = jax.random.randint(cap_key, (GROUP_SIZE,), CAP_FLOOR, SEQ_LEN + 1)
    full_dev = jax.random.randint(pick_key, (), 0, GROUP_SIZE)
    caps = jnp.where(jnp.arange(GROUP_SIZE) == full_dev, SEQ_LEN, caps)
    drawn = jax.random.randint(len_key, (GROUP_SIZE, B_DEV), LEN_FLOOR, caps[:, None] + 1)
    drawn = jnp.concatenate([drawn[:, 1:], caps[:, None]], axis=1)
    return jnp.sort(drawn, axis=1).reshape(BATCH).astype(jnp.int32)


def setup_inputs(seed: int = 0, part: int = 0) -> dict:
    part_key = jax.random.fold_in(jax.random.key(seed), part)
    x_key, len_key, cache_key = jax.random.split(part_key, 3)
    shared_keys = jax.random.split(jax.random.key(seed + 1), 7)
    wo_scale = (HEADS * LATENT) ** -0.5 * max(1.0, (SEQ_LEN / 64) ** 0.5)
    return {
        'x': jax.random.normal(x_key, (BATCH, D_MODEL), jnp.float32).astype(jnp.bfloat16),
        'lengths': draw_lengths(len_key),
        'cache': jax.random.normal(cache_key, (LAYERS, BATCH, SEQ_LEN, KV_DIM), jnp.float32).astype(jnp.bfloat16),
        'attn_gain': 0.5 + jax.random.uniform(shared_keys[0], (LAYERS, D_MODEL), jnp.float32),
        'ffn_gain': 0.5 + jax.random.uniform(shared_keys[1], (LAYERS, D_MODEL), jnp.float32),
        'w_query': (jax.random.normal(shared_keys[2], (LAYERS, D_MODEL, HEADS * KV_DIM), jnp.float32) * D_MODEL ** -0.5).astype(jnp.bfloat16),
        'w_attn_out': (jax.random.normal(shared_keys[3], (LAYERS, HEADS * LATENT, D_MODEL), jnp.float32) * wo_scale).astype(jnp.bfloat16),
        'w_up': (jax.random.normal(shared_keys[4], (LAYERS, D_MODEL, FF_DIM), jnp.float32) * D_MODEL ** -0.5).astype(jnp.bfloat16),
        'w_gate': (jax.random.normal(shared_keys[5], (LAYERS, D_MODEL, FF_DIM), jnp.float32) * D_MODEL ** -0.5).astype(jnp.bfloat16),
        'w_down': (jax.random.normal(shared_keys[6], (LAYERS, FF_DIM, D_MODEL), jnp.float32) * 2.0 * FF_DIM ** -0.5).astype(jnp.bfloat16),
    }


def rms_norm(rows, gain):
    rows_f = rows.astype(jnp.float32)
    mean_sq = jnp.mean(rows_f * rows_f, axis=-1, keepdims=True)
    return (rows_f * lax.rsqrt(mean_sq + NORM_EPS) * gain).astype(jnp.bfloat16)


def attention_layer(x_all, lengths, cache_l, gain, wq_l, wo_l):
    x_blocks = x_all.reshape(GROUP_SIZE, B_DEV, D_MODEL)
    len_blocks = lengths.reshape(GROUP_SIZE, B_DEV)
    cache_blocks = cache_l.reshape(GROUP_SIZE, B_DEV, SEQ_LEN, KV_DIM)
    positions = jnp.arange(SEQ_LEN)[None, None, :]

    def one_block(block):
        x_rows, len_rows, cache_rows = block
        normed = rms_norm(x_rows, gain)
        query = jnp.dot(normed, wq_l, preferred_element_type=jnp.float32).astype(jnp.bfloat16)
        query = query.reshape(B_DEV, HEADS, KV_DIM).astype(jnp.float32)
        cache_f = cache_rows.astype(jnp.float32)
        scores = jnp.einsum('bhc,btc->bht', query, cache_f) * SCORE_SCALE
        scores = jnp.where(positions < len_rows[:, None, None], scores, -jnp.inf)
        attn_probs = jax.nn.softmax(scores, axis=-1).astype(jnp.bfloat16).astype(jnp.float32)
        mixed = jnp.einsum('bht,btc->bhc', attn_probs, cache_f[:, :, :LATENT]).astype(jnp.bfloat16)
        attn_out = jnp.dot(mixed.reshape(B_DEV, HEADS * LATENT), wo_l, preferred_element_type=jnp.float32)
        return (x_rows.astype(jnp.float32) + attn_out).astype(jnp.bfloat16)

    return lax.map(one_block, (x_blocks, len_blocks, cache_blocks)).reshape(BATCH, D_MODEL)


def ffn_layer(x_all, gain, wu_l, wg_l, wd_l):
    normed = rms_norm(x_all, gain)
    gate_pre = jnp.dot(normed, wg_l, preferred_element_type=jnp.float32)
    up_pre = jnp.dot(normed, wu_l, preferred_element_type=jnp.float32)
    hidden = (jax.nn.silu(gate_pre) * up_pre).astype(jnp.bfloat16)
    ffn_out = jnp.dot(hidden, wd_l, preferred_element_type=jnp.float32)
    return (x_all.astype(jnp.float32) + ffn_out).astype(jnp.bfloat16)


def reference(x, lengths, cache, attn_gain, ffn_gain, w_query, w_attn_out, w_up, w_gate, w_down):
    def layer_step(x_cur, params):
        cache_l, gain_a, gain_f, wq_l, wo_l, wu_l, wg_l, wd_l = params
        x_cur = attention_layer(x_cur, lengths, cache_l, gain_a, wq_l, wo_l)
        x_cur = ffn_layer(x_cur, gain_f, wu_l, wg_l, wd_l)
        return x_cur, None

    x_final, _ = lax.scan(layer_step, x, (cache, attn_gain, ffn_gain, w_query, w_attn_out, w_up, w_gate, w_down))
    return x_final
```

```python
import functools

import jax
import jax.numpy as jnp
from jax import lax
from jax.experimental import pallas as pl
from jax.experimental.pallas import tpu as pltpu
from jax.sharding import PartitionSpec as P

NORM_EPS = 1e-6
BF = jnp.bfloat16
F32 = jnp.float32
GRP = 16
OBLK = 256


def kernel(dims, x_hbm, lens, cache_hbm, ga_ref, gf_ref, wq_hbm, wo_hbm, wu_hbm, wg_hbm, wd_hbm, out_hbm,
           r1, r2, r3, xfull, hbuf, q3, qs, sbuf, pbuf, o3, oall, xg, sown, prd, pst, hid, rb,
           sem_w, sem_c, sem_o, sem_f, sem_x, xi_s, xi_r, q_s, q_r, o_s, o_r, ag_s, ag_r, pd_s, pd_r, rs_s, rs_r,
           xx_s, xx_r):
    layers, rows, seq, kv, heads, latent, d, ff, chips = dims
    half = d // 2
    qh = heads * kv // 2
    qblk = qh // 4
    scale = (3 * (kv - latent)) ** -0.5
    n_grp = rows // GRP
    n_ob = half // OBLK
    n_lt = pl.cdiv(kv, 128)

    me = lax.axis_index('dp')
    c = lax.rem(me, 2)
    chip = me // 2
    partner = me + 1 - 2 * c
    right = lax.rem(chip + 1, chips) * 2 + c
    left = lax.rem(chip + chips - 1, chips) * 2 + c
    ch_r = lax.rem(chip + 1, chips)
    ch_l = lax.rem(chip + chips - 1, chips)
    ch_o = lax.rem(chip + 2, chips)

    def rc(src, dst, ss, rs, dev):
        return pltpu.make_async_remote_copy(src_ref=src, dst_ref=dst, send_sem=ss, recv_sem=rs,
                                            device_id={'dp': dev}, device_id_type=pl.DeviceIdType.MESH)

    def wq_copy(l, i):
        cols = pl.ds(pl.multiple_of(c * qh + i * qblk, 128), qblk)
        return pltpu.make_async_copy(wq_hbm.at[l, :, cols], r1.at[:, pl.ds(i * qblk, qblk)], sem_w.at[i])

    def c_copy(l, g):
        rs = pl.ds(pl.multiple_of(g * GRP, GRP), GRP)
        return pltpu.make_async_copy(cache_hbm.at[l, rs], r3.at[rs], sem_c.at[g])

    def wo_copy(l, nb):
        cols = pl.ds(pl.multiple_of(c * half + nb * OBLK, 128), OBLK)
        return pltpu.make_async_copy(wo_hbm.at[l, :, cols], r2.at[nb], sem_o.at[nb])

    def ffn_copies(l):
        lo = pl.ds(pl.multiple_of((1 - c) * half, 128), half)
        hi = pl.ds(pl.multiple_of(c * half, 128), half)
        return (
            pltpu.make_async_copy(wg_hbm.at[l], r1.at[:, pl.ds(0, ff)], sem_f.at[0]),
            pltpu.make_async_copy(wu_hbm.at[l], r1.at[:, pl.ds(ff, ff)], sem_f.at[1]),
            pltpu.make_async_copy(wd_hbm.at[l, :, lo], r1.at[pl.ds(0, ff), pl.ds(2 * ff, half)], sem_f.at[2]),
            pltpu.make_async_copy(wd_hbm.at[l, :, hi], r1.at[pl.ds(0, ff), pl.ds(2 * ff + half, half)], sem_f.at[3]),
        )

    x_in = [pltpu.make_async_copy(x_hbm.at[:, pl.ds(k * half, half)], xfull.at[k, pl.ds(0, rows)], sem_x.at[k])
            for k in range(2)]
    for cp in x_in:
        cp.start()
    for i in range(4):
        wq_copy(0, i).start()

    barrier = pltpu.get_barrier_semaphore()
    for dev in (partner, left, right):
        pl.semaphore_signal(barrier, inc=1, device_id={'dp': dev}, device_id_type=pl.DeviceIdType.MESH)
    pl.semaphore_wait(barrier, 3)

    x_out = [rc(x_hbm.at[:, pl.ds(k * half, half)], xfull.at[k, pl.ds(rows, rows)], xi_s.at[k], xi_r.at[k], partner)
             for k in range(2)]
    for cp in x_out:
        cp.start()
    for cp in x_in:
        cp.wait()
    for cp in x_out:
        cp.wait()

    def norm_rows(src, gain):
        scales = []
        for r in range(2 * rows // 16):
            a = src[0, pl.ds(r * 16, 16), :].astype(F32)
            b = src[1, pl.ds(r * 16, 16), :].astype(F32)
            ms = jnp.sum(a * a + b * b, axis=-1, keepdims=True) * (1.0 / d)
            scales.append(lax.rsqrt(ms + NORM_EPS))
        for r in range(2 * rows // 16):
            for k in range(2):
                a = src[k, pl.ds(r * 16, 16), :].astype(F32)
                hbuf[pl.ds(r * 16, 16), pl.ds(k * half, half)] = (
                    a * scales[r] * gain[:, k * half:(k + 1) * half]).astype(BF)

    def layer_body(l, carry):
        norm_rows(xfull, ga_ref[pl.ds(l, 1), :])
        q_sends = []
        for i in range(4):
            wq_copy(l, i).wait()

            @pl.when(l == 0)
            def _():
                if i < 2:
                    c_copy(0, 2 * i).start()
                    c_copy(0, 2 * i + 1).start()
                else:
                    wo_copy(0, 2 * (i - 2)).start()
                    wo_copy(0, 2 * (i - 2) + 1).start()

            acc = jnp.dot(hbuf[...], r1[:, i * qblk:(i + 1) * qblk], preferred_element_type=F32)
            acc = acc.astype(BF).astype(F32)
            rolled = pltpu.roll(acc, kv, 1)
            base = pl.multiple_of((c * (heads // 2) + 2 * i) * rows, rows)
            for t in range(n_lt):
                lanes = slice(t * 128, (t + 1) * 128)
                q3[t, pl.ds(base, rows), :] = acc[:rows, lanes]
                q3[t, pl.ds(base + rows, rows), :] = rolled[:rows, lanes]
                qs[t, pl.ds(2 * i * rows, rows), :] = acc[rows:, lanes]
                qs[t, pl.ds((2 * i + 1) * rows, rows), :] = rolled[rows:, lanes]
            cp = rc(qs.at[:, pl.ds(2 * i * rows, 2 * rows)], q3.at[:, pl.ds(base, 2 * rows)], q_s.at[i], q_r.at[i],
                    partner)
            cp.start()
            q_sends.append(cp)
        for cp in ffn_copies(l):
            cp.start()
        for cp in q_sends:
            cp.wait()

        def o_copy(g):
            src = oall.at[:, pl.ds(pl.multiple_of(g * GRP, GRP), GRP)]
            dst = oall.at[:, pl.ds(pl.multiple_of(rows + g * GRP, GRP), GRP)]
            return rc(src, dst, o_s.at[g], o_r.at[g], partner)

        pos = lax.broadcasted_iota(jnp.int32, (heads, seq), 1)
        first = lax.rem(lax.broadcasted_iota(jnp.int32, (GRP * heads, seq), 0), 2 * heads) < heads

        def attn_group(g, carry):
            c_copy(l, g).wait()
            for b in range(0, GRP, 2):
                row = g * GRP + b
                qb = jnp.concatenate(
                    [jnp.concatenate([q3[t, pl.ds(row + k, heads, stride=rows), :] for t in range(n_lt)], axis=1)
                     for k in range(2)], axis=0)
                keys = jnp.concatenate([r3[row], r3[row + 1]], axis=1)
                s = jnp.dot(qb[:, :kv].astype(BF), keys, preferred_element_type=F32) * scale
                sbuf[pl.ds(b * heads, heads), :] = jnp.where(pos < lens[row], s[:heads, :seq], -jnp.inf)
                sbuf[pl.ds((b + 1) * heads, heads), :] = jnp.where(pos < lens[row + 1], s[heads:, seq:], -jnp.inf)
            s = sbuf[...]
            e = jnp.exp(s - jnp.max(s, axis=-1, keepdims=True))
            p = e / jnp.sum(e, axis=-1, keepdims=True)
            pbuf[:, :seq] = jnp.where(first, p, 0.0).astype(BF)
            pbuf[:, seq:] = jnp.where(first, 0.0, p).astype(BF)
            for b in range(0, GRP, 2):
                row = g * GRP + b
                vals = jnp.concatenate([r3[row, 0:latent, :], r3[row + 1, 0:latent, :]], axis=1)
                o = lax.dot_general(pbuf[pl.ds(b * heads, 2 * heads), :], vals, (((1,), (1,)), ((), ())),
                                    preferred_element_type=F32)
                for t in range(latent // 128):
                    o3[t, pl.ds(b, heads, stride=GRP), :] = o[:heads, t * 128:(t + 1) * 128]
                    o3[t, pl.ds(b + 1, heads, stride=GRP), :] = o[heads:, t * 128:(t + 1) * 128]
            for t in range(latent // 128):
                oall[:, pl.ds(pl.multiple_of(g * GRP, GRP), GRP), t * 128:(t + 1) * 128] = (
                    o3[t].astype(BF).reshape(heads, GRP, 128))
            o_copy(g).start()
            return carry

        lax.fori_loop(0, n_grp, attn_group, 0)
        for g in range(n_grp):
            o_copy(g).wait()

        @pl.when(l + 1 < layers)
        def _():
            for g in range(n_grp):
                c_copy(l + 1, g).start()

        def out_block(nb, carry):
            wo_copy(l, nb).wait()
            cols = pl.ds(pl.multiple_of(nb * OBLK, OBLK), OBLK)
            acc = jnp.dot(oall[0], r2[nb, 0:latent, :], preferred_element_type=F32)
            for h in range(1, heads):
                acc = acc + jnp.dot(oall[h], r2[nb, h * latent:(h + 1) * latent, :], preferred_element_type=F32)
            xn = (xfull[c, :, cols].astype(F32) + acc).astype(BF)
            xg[chip, c, pl.ds(pl.multiple_of(c * rows, rows), rows), cols] = xn[:rows]
            xg[chip, c, pl.ds(pl.multiple_of((1 - c) * rows, rows), rows), cols] = xn[rows:]
            return carry

        lax.fori_loop(0, n_ob, out_block, 0)

        pa, pb = pl.ds(0, rows), pl.ds(rows, rows)

        def ag(k, ch, part, dev):
            ref = xg.at[ch, c] if part is None else xg.at[ch, c, part]
            return rc(ref, ref, ag_s.at[k], ag_r.at[k], dev)

        def ag_in(k, ch, half_ix, part):
            ref = xg.at[ch, half_ix] if part is None else xg.at[ch, half_ix, part]
            return rc(ref, ref, ag_s.at[k], ag_r.at[k], partner)

        sends = [ag(0, chip, None, partner), ag(1, chip, pa, right), ag(3, chip, pb, left),
                 ag(2, chip, pb, right), ag(4, chip, pa, left)]
        fwd = [ag(5, ch_l, pa, right), ag(6, ch_r, pb, left), ag(7, ch_l, None, partner),
               ag(8, ch_r, None, partner), ag(9, ch_o, None, partner)]
        for cp in sends:
            cp.start()

        @pl.when(l + 1 < layers)
        def _():
            for nb in range(n_ob):
                wo_copy(l + 1, nb).start()

        ra, rbb = pl.ds(0, rows), pl.ds(rows, rows)
        rs_copies = [
            rc(sown.at[1, rbb], rb.at[0], rs_s.at[0], rs_r.at[0], right),
            rc(sown.at[2, ra], rb.at[1], rs_s.at[1], rs_r.at[1], left),
            rc(sown.at[3, ra], rb.at[2], rs_s.at[2], rs_r.at[2], right),
            rc(sown.at[3, rbb], rb.at[3], rs_s.at[3], rs_r.at[3], left),
            rc(sown.at[1, ra], rb.at[4], rs_s.at[4], rs_r.at[4], right),
            rc(sown.at[2, rbb], rb.at[5], rs_s.at[5], rs_r.at[5], left),
        ]

        def pd_copy(k):
            return rc(pst.at[lax.rem(k, 2)], prd.at[k], pd_s.at[k], pd_r.at[k], partner)

        def pair_sum(k):
            pd_copy(k).wait_recv()
            sown[k] = sown[k] + prd[k]

        for cp in ffn_copies(l):
            cp.wait()

        def chunk(k, carry):
            j = lax.rem(chip + k * (k + 1) // 2, chips)

            @pl.when(k == 0)
            def _():
                ag_in(0, chip, 1 - c, None).wait_recv()

            @pl.when(k == 1)
            def _():
                ag_in(1, ch_l, c, pa).wait_recv()
                fwd[0].start()
                ag_in(3, ch_r, c, pb).wait_recv()
                fwd[1].start()
                ag_in(4, ch_r, c, pa).wait_recv()
                fwd[3].start()
                ag_in(2, ch_l, c, pb).wait_recv()
                fwd[2].start()
                ag_in(8, ch_r, 1 - c, None).wait_recv()

            @pl.when(k == 2)
            def _():
                ag_in(7, ch_l, 1 - c, None).wait_recv()

            @pl.when(k == 3)
            def _():
                ag_in(9, ch_o, 1 - c, None).wait_recv()

            norm_rows(xg.at[j], gf_ref[pl.ds(l, 1), :])
            for lo in range(0, ff, 512):
                w = min(512, ff - lo)
                gate = jnp.dot(hbuf[...], r1[:, lo:lo + w], preferred_element_type=F32)
                up = jnp.dot(hbuf[...], r1[:, ff + lo:ff + lo + w], preferred_element_type=F32)
                hid[:, lo:lo + w] = (jax.nn.silu(gate) * up).astype(BF)

            @pl.when(k == 1)
            def _():
                pair_sum(0)

            @pl.when(k == 2)
            def _():
                pair_sum(1)
                rs_copies[0].start()
                ag_in(5, ch_o, c, pa).wait_recv()
                ag_in(6, ch_o, c, pb).wait_recv()
                fwd[4].start()

            @pl.when(k == 3)
            def _():
                pair_sum(2)
                rs_copies[1].start()

            @pl.when(k >= 2)
            def _():
                pd_copy(k - 2).wait_send()

            slot = lax.rem(k, 2)
            for lo in range(0, half, 512):
                pst[slot, :, lo:lo + 512] = jnp.dot(
                    hid[...], r1[0:ff, 2 * ff + lo:2 * ff + lo + 512], preferred_element_type=F32)
            pd_copy(k).start()
            for lo in range(0, half, 512):
                sown[k, :, lo:lo + 512] = jnp.dot(
                    hid[...], r1[0:ff, 2 * ff + half + lo:2 * ff + half + lo + 512], preferred_element_type=F32)
            return carry

        lax.fori_loop(0, chips, chunk, 0)

        @pl.when(l + 1 < layers)
        def _():
            for i in range(4):
                wq_copy(l + 1, i).start()

        for cp in sends + fwd:
            cp.wait_send()
        pair_sum(3)
        rs_copies[2].start()
        rs_copies[3].start()
        rs_copies[2].wait_recv()
        sown[1, ra] = sown[1, ra] + rb[2]
        rs_copies[4].start()
        rs_copies[3].wait_recv()
        sown[2, rbb] = sown[2, rbb] + rb[3]
        rs_copies[5].start()
        pd_copy(2).wait_send()
        pd_copy(3).wait_send()
        rs_copies[0].wait_recv()
        rs_copies[1].wait_recv()
        sown[0, ra] = sown[0, ra] + rb[1]
        sown[0, rbb] = sown[0, rbb] + rb[0]
        rs_copies[4].wait_recv()
        rs_copies[5].wait_recv()
        mine = pl.ds(pl.multiple_of(c * rows, rows), rows)
        other = pl.ds(pl.multiple_of((1 - c) * rows, rows), rows)
        rb[4] = sown[0, ra] + rb[4] + xg[chip, c, ra].astype(F32)
        rb[5] = sown[0, rbb] + rb[5] + xg[chip, c, rbb].astype(F32)
        xfull[c, pl.ds(0, rows)] = rb[4 + c].astype(BF)
        xfull[c, pl.ds(rows, rows)] = rb[5 - c].astype(BF)
        xx = [rc(xfull.at[c, pl.ds(rows, rows)], xfull.at[c, pl.ds(0, rows)], xx_s.at[0], xx_r.at[0], partner),
              rc(xfull.at[c, pl.ds(0, rows)], xfull.at[c, pl.ds(rows, rows)], xx_s.at[1], xx_r.at[1], partner)]
        for cp in xx:
            cp.start()
        for cp in rs_copies:
            cp.wait_send()
        for cp in xx:
            cp.wait()
        return carry

    lax.fori_loop(0, layers, layer_body, 0)
    x_fin = [pltpu.make_async_copy(xfull.at[k, pl.ds(0, rows)], out_hbm.at[:, pl.ds(k * half, half)], sem_x.at[k])
             for k in range(2)]
    for cp in x_fin:
        cp.start()
    for cp in x_fin:
        cp.wait()


def solution(mesh):
    row_axes = ('replica', 'dp')
    n = mesh.shape['dp']
    chips = n // 2

    def local_step(x_rows, len_rows, cache, attn_gain, ffn_gain, w_query, w_attn_out, w_up, w_gate, w_down):
        layers, rows, seq, kv = cache.shape
        d = x_rows.shape[1]
        heads = w_query.shape[2] // kv
        latent = w_attn_out.shape[1] // heads
        ff = w_up.shape[2]
        half = d // 2
        qh = heads * kv // 2
        dims = (layers, rows, seq, kv, heads, latent, d, ff, chips)
        n_grp = rows // GRP
        n_ob = half // OBLK
        n_lt = pl.cdiv(kv, 128)
        any_spec = pl.BlockSpec(memory_space=pl.ANY)
        vmem = pl.BlockSpec(memory_space=pltpu.VMEM)
        dma = pltpu.SemaphoreType.DMA
        return pl.pallas_call(
            functools.partial(kernel, dims),
            out_shape=jax.ShapeDtypeStruct(x_rows.shape, x_rows.dtype),
            in_specs=[any_spec, pl.BlockSpec(memory_space=pltpu.SMEM), any_spec, vmem, vmem] + [any_spec] * 5,
            out_specs=any_spec,
            scratch_shapes=[
                pltpu.VMEM((d, max(qh, 2 * ff + d)), BF),
                pltpu.VMEM((n_ob, heads * latent, OBLK), BF),
                pltpu.VMEM((rows, kv, seq), BF),
                pltpu.VMEM((2, 2 * rows, half), BF),
                pltpu.VMEM((2 * rows, d), BF),
                pltpu.VMEM((n_lt, heads * rows, 128), F32),
                pltpu.VMEM((n_lt, heads // 2 * rows, 128), F32),
                pltpu.VMEM((GRP * heads, seq), F32),
                pltpu.VMEM((GRP * heads, 2 * seq), BF),
                pltpu.VMEM((latent // 128, GRP * heads, 128), F32),
                pltpu.VMEM((heads, 2 * rows, latent), BF),
                pltpu.VMEM((chips, 2, 2 * rows, half), BF),
                pltpu.VMEM((chips, 2 * rows, half), F32),
                pltpu.VMEM((chips, 2 * rows, half), F32),
                pltpu.VMEM((2, 2 * rows, half), F32),
                pltpu.VMEM((2 * rows, ff), BF),
                pltpu.VMEM((6, rows, half), F32),
                dma((4,)), dma((n_grp,)), dma((n_ob,)), dma((4,)), dma((2,)),
                dma((2,)), dma((2,)), dma((4,)), dma((4,)), dma((n_grp,)), dma((n_grp,)),
                dma((10,)), dma((10,)), dma((chips,)), dma((chips,)), dma((6,)), dma((6,)),
                dma((2,)), dma((2,)),
            ],
            compiler_params=pltpu.CompilerParams(
                collective_id=0, has_side_effects=True, vmem_limit_bytes=67043328),
        )(x_rows, len_rows, jnp.swapaxes(cache, 2, 3), attn_gain, ffn_gain, w_query, w_attn_out, w_up, w_gate, w_down)

    return jax.shard_map(
        local_step,
        mesh=mesh,
        in_specs=(P(row_axes, None), P(row_axes), P(None, row_axes, None, None), P(), P(), P(), P(),
                  P(None, None, 'dp'), P(None, None, 'dp'), P(None, 'dp', None)),
        out_specs=P(row_axes, None),
        check_vma=False,
    )
```

```python
import functools

import jax
import jax.numpy as jnp
from jax import lax
from jax.experimental import pallas as pl
from jax.experimental.pallas import tpu as pltpu
from jax.sharding import PartitionSpec as P

NORM_EPS = 1e-6
BF = jnp.bfloat16
F32 = jnp.float32
GRP = 16
OBLK = 256


def kernel(dims, x_hbm, len_hbm, cache_hbm, ga_hbm, gf_hbm, wq_hbm, wo_hbm, wu_hbm, wg_hbm, wd_hbm, out_hbm,
           lens, ga_ref, gf_ref, r1, r2, r3, xfull, hbuf, q3, qs, sbuf, pbuf, o3, oall, xg, sown, prd, pst, hid, rb,
           sem_p, sem_w, sem_c, sem_o, sem_f, sem_x, xi_s, xi_r, q_s, q_r, o_s, o_r, ag_s, ag_r, pd_s, pd_r, rs_s, rs_r,
           xx_s, xx_r):
    layers, rows, seq, kv, heads, latent, d, ff, chips = dims
    half = d // 2
    qh = heads * kv // 2
    qblk = qh // 4
    scale = (3 * (kv - latent)) ** -0.5
    n_grp = rows // GRP
    n_ob = half // OBLK
    n_lt = pl.cdiv(kv, 128)

    me = lax.axis_index('dp')
    c = lax.rem(me, 2)
    chip = me // 2
    partner = me + 1 - 2 * c
    right = lax.rem(chip + 1, chips) * 2 + c
    left = lax.rem(chip + chips - 1, chips) * 2 + c
    ch_r = lax.rem(chip + 1, chips)
    ch_l = lax.rem(chip + chips - 1, chips)
    ch_o = lax.rem(chip + 2, chips)

    def rc(src, dst, ss, rs, dev):
        return pltpu.make_async_remote_copy(src_ref=src, dst_ref=dst, send_sem=ss, recv_sem=rs,
                                            device_id={'dp': dev}, device_id_type=pl.DeviceIdType.MESH)

    def wq_copy(l, i):
        cols = pl.ds(pl.multiple_of(c * qh + i * qblk, 128), qblk)
        return pltpu.make_async_copy(wq_hbm.at[l, :, cols], r1.at[:, pl.ds(i * qblk, qblk)], sem_w.at[i])

    def c_copy(l, g):
        rs = pl.ds(pl.multiple_of(g * GRP, GRP), GRP)
        return pltpu.make_async_copy(cache_hbm.at[l, rs], r3.at[rs], sem_c.at[g])

    def wo_copy(l, nb):
        cols = pl.ds(pl.multiple_of(c * half + nb * OBLK, 128), OBLK)
        return pltpu.make_async_copy(wo_hbm.at[l, :, cols], r2.at[nb], sem_o.at[nb])

    def ffn_copies(l):
        lo = pl.ds(pl.multiple_of((1 - c) * half, 128), half)
        hi = pl.ds(pl.multiple_of(c * half, 128), half)
        return (
            pltpu.make_async_copy(wg_hbm.at[l], r1.at[:, pl.ds(0, ff)], sem_f.at[0]),
            pltpu.make_async_copy(wu_hbm.at[l], r1.at[:, pl.ds(ff, ff)], sem_f.at[1]),
            pltpu.make_async_copy(wd_hbm.at[l, :, lo], r1.at[pl.ds(0, ff), pl.ds(2 * ff, half)], sem_f.at[2]),
            pltpu.make_async_copy(wd_hbm.at[l, :, hi], r1.at[pl.ds(0, ff), pl.ds(2 * ff + half, half)], sem_f.at[3]),
        )

    barrier = pltpu.get_barrier_semaphore()
    for dev in (partner, left, right):
        pl.semaphore_signal(barrier, inc=1, device_id={'dp': dev}, device_id_type=pl.DeviceIdType.MESH)
    x_in = [pltpu.make_async_copy(x_hbm.at[:, pl.ds(k * half, half)], xfull.at[k, pl.ds(0, rows)], sem_x.at[k])
            for k in range(2)]
    x_out = [rc(xfull.at[k, pl.ds(0, rows)], xfull.at[k, pl.ds(rows, rows)], xi_s.at[k], xi_r.at[k], partner)
             for k in range(2)]
    small = [pltpu.make_async_copy(ga_hbm, ga_ref, sem_p.at[0]), pltpu.make_async_copy(gf_hbm, gf_ref, sem_p.at[1]),
             pltpu.make_async_copy(len_hbm, lens, sem_p.at[2])]
    for cp in x_in + small:
        cp.start()
    for i in range(4):
        wq_copy(0, i).start()
    pl.semaphore_wait(barrier, 3)
    for k in range(2):
        x_in[k].wait()
        x_out[k].start()
    for cp in small + x_out:
        cp.wait()

    def norm_rows(piece, gain):
        scales = []
        for r in range(2 * rows // 16):
            a, b = (piece(k, r * 16).astype(F32) for k in range(2))
            ms = jnp.sum(a * a + b * b, axis=-1, keepdims=True) * (1.0 / d)
            scales.append(lax.rsqrt(ms + NORM_EPS))
        for r in range(2 * rows // 16):
            for k in range(2):
                hbuf[pl.ds(r * 16, 16), pl.ds(k * half, half)] = (
                    piece(k, r * 16).astype(F32) * scales[r] * gain[:, k * half:(k + 1) * half]).astype(BF)

    def layer_body(l, carry):
        norm_rows(lambda k, r: xfull[k, pl.ds(r, 16), :], ga_ref[pl.ds(l, 1), :])
        q_sends = []
        for i in range(4):
            wq_copy(l, i).wait()

            @pl.when(l == 0)
            def _():
                if i < 2:
                    c_copy(0, 2 * i).start()
                    c_copy(0, 2 * i + 1).start()
                else:
                    wo_copy(0, 2 * (i - 2)).start()
                    wo_copy(0, 2 * (i - 2) + 1).start()

            acc = jnp.dot(hbuf[...], r1[:, i * qblk:(i + 1) * qblk], preferred_element_type=F32)
            acc = acc.astype(BF).astype(F32)
            rolled = pltpu.roll(acc, kv, 1)
            base = pl.multiple_of((c * (heads // 2) + 2 * i) * rows, rows)
            for t in range(n_lt):
                lanes = slice(t * 128, (t + 1) * 128)
                q3[t, pl.ds(base, rows), :] = acc[:rows, lanes]
                q3[t, pl.ds(base + rows, rows), :] = rolled[:rows, lanes]
                qs[t, pl.ds(2 * i * rows, rows), :] = acc[rows:, lanes]
                qs[t, pl.ds((2 * i + 1) * rows, rows), :] = rolled[rows:, lanes]
            cp = rc(qs.at[:, pl.ds(2 * i * rows, 2 * rows)], q3.at[:, pl.ds(base, 2 * rows)], q_s.at[i], q_r.at[i],
                    partner)
            cp.start()
            q_sends.append(cp)
        for cp in ffn_copies(l):
            cp.start()
        for cp in q_sends:
            cp.wait()

        def o_copy(g):
            src = oall.at[:, pl.ds(pl.multiple_of(g * GRP, GRP), GRP)]
            dst = oall.at[:, pl.ds(pl.multiple_of(rows + g * GRP, GRP), GRP)]
            return rc(src, dst, o_s.at[g], o_r.at[g], partner)

        pos = lax.broadcasted_iota(jnp.int32, (heads, seq), 1)
        first = lax.rem(lax.broadcasted_iota(jnp.int32, (GRP * heads, seq), 0), 2 * heads) < heads

        def scores(g, b):
            row = g * GRP + b
            qb = jnp.concatenate(
                [jnp.concatenate([q3[t, pl.ds(row + k, heads, stride=rows), :] for t in range(n_lt)], axis=1)
                 for k in range(2)], axis=0)
            keys = jnp.concatenate([r3[row], r3[row + 1]], axis=1)
            s = jnp.dot(qb[:, :kv].astype(BF), keys, preferred_element_type=F32) * scale
            sbuf[g % 2, pl.ds(b * heads, heads), :] = jnp.where(pos < lens[row], s[:heads, :seq], -jnp.inf)
            sbuf[g % 2, pl.ds((b + 1) * heads, heads), :] = jnp.where(pos < lens[row + 1], s[heads:, seq:], -jnp.inf)

        def mix(g, b):
            row = g * GRP + b
            vals = jnp.concatenate([r3[row, 0:latent, :], r3[row + 1, 0:latent, :]], axis=1)
            o = lax.dot_general(pbuf[pl.ds(b * heads, 2 * heads), :], vals, (((1,), (1,)), ((), ())),
                                preferred_element_type=F32)
            for t in range(latent // 128):
                o3[t, pl.ds(b, heads, stride=GRP), :] = o[:heads, t * 128:(t + 1) * 128]
                o3[t, pl.ds(b + 1, heads, stride=GRP), :] = o[heads:, t * 128:(t + 1) * 128]

        c_copy(l, 0).wait()
        for b in range(0, GRP, 2):
            scores(0, b)
        for g in range(n_grp):
            if g + 1 < n_grp:
                c_copy(l, g + 1).wait()
            s = sbuf[g % 2]
            e = jnp.exp(s - jnp.max(s, axis=-1, keepdims=True))
            p = e / jnp.sum(e, axis=-1, keepdims=True)
            pbuf[:, :seq] = jnp.where(first, p, 0.0).astype(BF)
            pbuf[:, seq:] = jnp.where(first, 0.0, p).astype(BF)
            for b in range(0, GRP, 2):
                if g + 1 < n_grp:
                    scores(g + 1, b)
                mix(g, b)
            for t in range(latent // 128):
                oall[:, pl.ds(g * GRP, GRP), t * 128:(t + 1) * 128] = o3[t].astype(BF).reshape(heads, GRP, 128)
            o_copy(g).start()
        for g in range(n_grp):
            o_copy(g).wait()

        @pl.when(l + 1 < layers)
        def _():
            for g in range(n_grp):
                c_copy(l + 1, g).start()

        pa, pb = pl.ds(0, rows), pl.ds(rows, rows)
        hc = half // 2

        def ag(k, ch, part, dev, hx=None, cols=None):
            hx = c if hx is None else hx
            ref = xg.at[ch, hx] if part is None else xg.at[ch, hx, part]
            if cols is not None:
                ref = xg.at[ch, hx, part, pl.ds(cols * hc, hc)]
            return rc(ref, ref, ag_s.at[k], ag_r.at[k], dev)

        sends = [ag(0, chip, pa, right, cols=0), ag(1, chip, pb, left, cols=0),
                 ag(2, chip, pa, right, cols=1), ag(3, chip, pb, left, cols=1), ag(4, chip, None, partner),
                 ag(5, chip, pb, right), ag(6, chip, pa, left)]
        fwd = [ag(7, ch_l, pa, right), ag(8, ch_r, pb, left), ag(9, ch_l, pa, partner), ag(10, ch_r, pb, partner),
               ag(11, ch_l, pb, partner), ag(12, ch_r, pa, partner), ag(13, ch_o, pa, partner),
               ag(14, ch_o, pb, partner)]

        def got(k, ch, part, hx=None, cols=None):
            ag(k, ch, part, partner, hx, cols).wait_recv()

        for nb in range(n_ob):
            wo_copy(l, nb).wait()
            cols = pl.ds(nb * OBLK, OBLK)
            acc = jnp.dot(oall[0], r2[nb, 0:latent, :], preferred_element_type=F32)
            for h in range(1, heads):
                acc = acc + jnp.dot(oall[h], r2[nb, h * latent:(h + 1) * latent, :], preferred_element_type=F32)
            xn = (xfull[c, :, cols].astype(F32) + acc).astype(BF)
            xg[chip, c, pl.ds(pl.multiple_of(c * rows, rows), rows), cols] = xn[:rows]
            xg[chip, c, pl.ds(pl.multiple_of((1 - c) * rows, rows), rows), cols] = xn[rows:]
            if nb == n_ob // 2 - 1:
                sends[0].start()
                sends[1].start()
        for cp in sends[2:]:
            cp.start()

        @pl.when(l + 1 < layers)
        def _():
            for nb in range(n_ob):
                wo_copy(l + 1, nb).start()

        hr = rows // 2

        def rs_sub(slot, dst, base, sub, k, dev):
            return rc(sown.at[slot, pl.ds(base + sub * hr, hr)], rb.at[dst, pl.ds(sub * hr, hr)],
                      rs_s.at[k], rs_r.at[k], dev)

        unm = [rc(sown.at[1, pa], rb.at[0], rs_s.at[0], rs_r.at[0], left),
               rc(sown.at[1, pb], rb.at[1], rs_s.at[1], rs_r.at[1], right)]
        rly = [rs_sub(2, 2, 0, 0, 2, right), rs_sub(2, 3, rows, 0, 3, left),
               rs_sub(2, 2, 0, 1, 4, right), rs_sub(2, 3, rows, 1, 5, left)]
        mrg = [rs_sub(3, 4, 0, 0, 6, right), rs_sub(3, 5, rows, 0, 7, left),
               rs_sub(3, 4, 0, 1, 8, right), rs_sub(3, 5, rows, 1, 9, left)]

        def pd_copy(k):
            return rc(pst.at[lax.rem(k, 2)], prd.at[k], pd_s.at[k], pd_r.at[k], partner)

        def pair_sum(k):
            pd_copy(k).wait_recv()
            sown[k] = sown[k] + prd[k]

        for cp in ffn_copies(l):
            cp.wait()

        def chunk(k, carry):
            p0 = lax.rem(chip + chips - k, chips)
            p1 = lax.rem(chip + k, chips)

            @pl.when(k == 0)
            def _():
                got(4, chip, None, 1 - c)

            @pl.when(k == 1)
            def _():
                got(0, ch_l, pa, cols=0)
                got(2, ch_l, pa, cols=1)
                fwd[0].start()
                fwd[2].start()
                got(1, ch_r, pb, cols=0)
                got(3, ch_r, pb, cols=1)
                fwd[1].start()
                fwd[3].start()
                pair_sum(0)
                got(9, ch_l, pa, 1 - c)
                got(10, ch_r, pb, 1 - c)

            @pl.when(k == 2)
            def _():
                pair_sum(1)
                unm[0].start()
                unm[1].start()
                got(7, ch_o, pa)
                fwd[6].start()
                got(8, ch_o, pb)
                fwd[7].start()
                got(13, ch_o, pa, 1 - c)
                got(14, ch_o, pb, 1 - c)

            @pl.when(k == 3)
            def _():
                pair_sum(2)
                for cp in rly:
                    cp.start()
                got(11, ch_l, pb, 1 - c)
                got(12, ch_r, pa, 1 - c)

            norm_rows(lambda h, r: xg[p0 if r < rows else p1, h, pl.ds(r, 16), :], gf_ref[pl.ds(l, 1), :])
            for lo in range(0, ff, 512):
                w = min(512, ff - lo)
                gate = jnp.dot(hbuf[...], r1[:, lo:lo + w], preferred_element_type=F32)
                up = jnp.dot(hbuf[...], r1[:, ff + lo:ff + lo + w], preferred_element_type=F32)
                hid[:, lo:lo + w] = (jax.nn.silu(gate) * up).astype(BF)

            @pl.when(k == 1)
            def _():
                got(5, ch_l, pb)
                fwd[4].start()
                got(6, ch_r, pa)
                fwd[5].start()

            @pl.when(k >= 2)
            def _():
                pd_copy(k - 2).wait_send()

            slot = lax.rem(k, 2)
            for lo in range(0, half, 512):
                pst[slot, :, lo:lo + 512] = jnp.dot(
                    hid[...], r1[0:ff, 2 * ff + lo:2 * ff + lo + 512], preferred_element_type=F32)
            pd_copy(k).start()
            for lo in range(0, half, 512):
                sown[k, :, lo:lo + 512] = jnp.dot(
                    hid[...], r1[0:ff, 2 * ff + half + lo:2 * ff + half + lo + 512], preferred_element_type=F32)
            return carry

        lax.fori_loop(0, chips, chunk, 0)

        @pl.when(l + 1 < layers)
        def _():
            for i in range(4):
                wq_copy(l + 1, i).start()

        for cp in sends + fwd:
            cp.wait_send()
        pair_sum(3)
        for i in range(4):
            sub = pl.ds((i // 2) * hr, hr)
            dst = pl.ds((i % 2) * rows + (i // 2) * hr, hr)
            rly[i].wait_recv()
            sown[3, dst] = sown[3, dst] + rb[2 + i % 2, sub]
            mrg[i].start()
        pd_copy(2).wait_send()
        pd_copy(3).wait_send()
        unm[0].wait_recv()
        unm[1].wait_recv()
        rb[0] = rb[0] + sown[0, pa] + xg[chip, c, pa].astype(F32)
        rb[1] = rb[1] + sown[0, pb] + xg[chip, c, pb].astype(F32)
        for cp in mrg:
            cp.wait_recv()
        xfull[c, pl.ds(0, rows)] = (rb[c] + rb[4 + c]).astype(BF)
        xfull[c, pl.ds(rows, rows)] = (rb[1 - c] + rb[5 - c]).astype(BF)
        xx = [rc(xfull.at[c, pl.ds(rows, rows)], xfull.at[c, pl.ds(0, rows)], xx_s.at[0], xx_r.at[0], partner),
              rc(xfull.at[c, pl.ds(0, rows)], xfull.at[c, pl.ds(rows, rows)], xx_s.at[1], xx_r.at[1], partner)]
        for cp in xx:
            cp.start()
        for cp in unm + rly + mrg:
            cp.wait_send()
        for cp in xx:
            cp.wait()
        return carry

    lax.fori_loop(0, layers, layer_body, 0)
    x_fin = [pltpu.make_async_copy(xfull.at[k, pl.ds(0, rows)], out_hbm.at[:, pl.ds(k * half, half)], sem_x.at[k])
             for k in range(2)]
    for cp in x_fin:
        cp.start()
    for cp in x_fin:
        cp.wait()


def solution(mesh):
    row_axes = ('replica', 'dp')
    n = mesh.shape['dp']
    chips = n // 2

    def local_step(x_rows, len_rows, cache, attn_gain, ffn_gain, w_query, w_attn_out, w_up, w_gate, w_down):
        layers, rows, seq, kv = cache.shape
        d = x_rows.shape[1]
        heads = w_query.shape[2] // kv
        latent = w_attn_out.shape[1] // heads
        ff = w_up.shape[2]
        half = d // 2
        qh = heads * kv // 2
        dims = (layers, rows, seq, kv, heads, latent, d, ff, chips)
        n_grp = rows // GRP
        n_ob = half // OBLK
        n_lt = pl.cdiv(kv, 128)
        any_spec = pl.BlockSpec(memory_space=pl.ANY)
        dma = pltpu.SemaphoreType.DMA
        return pl.pallas_call(
            functools.partial(kernel, dims),
            out_shape=jax.ShapeDtypeStruct(x_rows.shape, x_rows.dtype),
            in_specs=[any_spec] * 10,
            out_specs=any_spec,
            scratch_shapes=[
                pltpu.SMEM((rows,), jnp.int32),
                pltpu.VMEM(attn_gain.shape, F32),
                pltpu.VMEM(ffn_gain.shape, F32),
                pltpu.VMEM((d, max(qh, 2 * ff + d)), BF),
                pltpu.VMEM((n_ob, heads * latent, OBLK), BF),
                pltpu.VMEM((rows, kv, seq), BF),
                pltpu.VMEM((2, 2 * rows, half), BF),
                pltpu.VMEM((2 * rows, d), BF),
                pltpu.VMEM((n_lt, heads * rows, 128), F32),
                pltpu.VMEM((n_lt, heads // 2 * rows, 128), F32),
                pltpu.VMEM((2, GRP * heads, seq), F32),
                pltpu.VMEM((GRP * heads, 2 * seq), BF),
                pltpu.VMEM((latent // 128, GRP * heads, 128), F32),
                pltpu.VMEM((heads, 2 * rows, latent), BF),
                pltpu.VMEM((chips, 2, 2 * rows, half), BF),
                pltpu.VMEM((chips, 2 * rows, half), F32),
                pltpu.VMEM((chips, 2 * rows, half), F32),
                pltpu.VMEM((2, 2 * rows, half), F32),
                pltpu.VMEM((2 * rows, ff), BF),
                pltpu.VMEM((6, rows, half), F32),
                dma((3,)), dma((4,)), dma((n_grp,)), dma((n_ob,)), dma((4,)), dma((2,)),
                dma((2,)), dma((2,)), dma((4,)), dma((4,)), dma((n_grp,)), dma((n_grp,)),
                dma((15,)), dma((15,)), dma((chips,)), dma((chips,)), dma((10,)), dma((10,)),
                dma((2,)), dma((2,)),
            ],
            compiler_params=pltpu.CompilerParams(
                collective_id=0, has_side_effects=True, vmem_limit_bytes=67043328),
        )(x_rows, len_rows, jnp.swapaxes(cache, 2, 3), attn_gain, ffn_gain, w_query, w_attn_out, w_up, w_gate, w_down)

    return jax.shard_map(
        local_step,
        mesh=mesh,
        in_specs=(P(row_axes, None), P(row_axes), P(None, row_axes, None, None), P(), P(), P(), P(),
                  P(None, None, 'dp'), P(None, None, 'dp'), P(None, 'dp', None)),
        out_specs=P(row_axes, None),
        check_vma=False,
    )
```

```python
import functools

import jax
import jax.numpy as jnp
from jax import lax
from jax.experimental import pallas as pl
from jax.experimental.pallas import tpu as pltpu
from jax.sharding import PartitionSpec as P

NORM_EPS = 1e-6
BF = jnp.bfloat16
F32 = jnp.float32
GRP = 16
OBLK = 256


def kernel(dims, x_hbm, len_hbm, cache_hbm, ga_hbm, gf_hbm, wq_hbm, wo_hbm, wu_hbm, wg_hbm, wd_hbm, out_hbm,
           lens, ga_ref, gf_ref, r1, r2, r3, xfull, hbuf, q3, qs, sbuf, pbuf, o3, oall, xg, sown, prd, pst, hid, rb,
           sem_p, sem_w, sem_c, sem_o, sem_f, sem_x, xi_s, xi_r, q_s, q_r, o_s, o_r, af_s, af_r, ag_s, ag_r, pd_s, pd_r, rs_s, rs_r,
           xx_s, xx_r):
    layers, rows, seq, kv, heads, latent, d, ff, chips = dims
    half = d // 2
    qh = heads * kv // 2
    qsplit = ((0, heads // 4), (heads // 4, heads // 8), (3 * heads // 8, heads // 8))
    scale = (3 * (kv - latent)) ** -0.5
    n_grp = rows // GRP
    n_ob = half // OBLK
    n_lt = pl.cdiv(kv, 128)

    me = lax.axis_index('dp')
    c = lax.rem(me, 2)
    chip = me // 2
    partner = me + 1 - 2 * c
    right = lax.rem(chip + 1, chips) * 2 + c
    left = lax.rem(chip + chips - 1, chips) * 2 + c
    ch_r = lax.rem(chip + 1, chips)
    ch_l = lax.rem(chip + chips - 1, chips)
    ch_o = lax.rem(chip + 2, chips)

    def rc(src, dst, ss, rs, dev):
        return pltpu.make_async_remote_copy(src_ref=src, dst_ref=dst, send_sem=ss, recv_sem=rs,
                                            device_id={'dp': dev}, device_id_type=pl.DeviceIdType.MESH)

    def wq_copy(l, i):
        lo, w = qsplit[i][0] * kv, qsplit[i][1] * kv
        cols = pl.ds(pl.multiple_of(c * qh + lo, 128), w)
        return pltpu.make_async_copy(wq_hbm.at[l, :, cols], r1.at[:, pl.ds(lo, w)], sem_w.at[i])

    def c_copy(l, g):
        rs = pl.ds(pl.multiple_of(g * GRP, GRP), GRP)
        return pltpu.make_async_copy(cache_hbm.at[l, rs], r3.at[rs], sem_c.at[g])

    def wo_copy(l, nb):
        cols = pl.ds(pl.multiple_of(c * half + nb * OBLK, 128), OBLK)
        return pltpu.make_async_copy(wo_hbm.at[l, :, cols], r2.at[nb], sem_o.at[nb])

    def ffn_copies(l):
        lo = pl.ds(pl.multiple_of((1 - c) * half, 128), half)
        hi = pl.ds(pl.multiple_of(c * half, 128), half)
        return (
            pltpu.make_async_copy(wg_hbm.at[l], r1.at[:, pl.ds(0, ff)], sem_f.at[0]),
            pltpu.make_async_copy(wu_hbm.at[l], r1.at[:, pl.ds(ff, ff)], sem_f.at[1]),
            pltpu.make_async_copy(wd_hbm.at[l, :, lo], r1.at[pl.ds(0, ff), pl.ds(2 * ff, half)], sem_f.at[2]),
            pltpu.make_async_copy(wd_hbm.at[l, :, hi], r1.at[pl.ds(0, ff), pl.ds(2 * ff + half, half)], sem_f.at[3]),
        )

    barrier = pltpu.get_barrier_semaphore()
    for dev in (partner, left, right):
        pl.semaphore_signal(barrier, inc=1, device_id={'dp': dev}, device_id_type=pl.DeviceIdType.MESH)
    x_in = [pltpu.make_async_copy(x_hbm.at[:, pl.ds(k * half, half)], xfull.at[k, pl.ds(0, rows)], sem_x.at[k])
            for k in range(2)]
    x_out = [rc(xfull.at[k, pl.ds(0, rows)], xfull.at[k, pl.ds(rows, rows)], xi_s.at[k], xi_r.at[k], partner)
             for k in range(2)]
    small = [pltpu.make_async_copy(ga_hbm, ga_ref, sem_p.at[0]), pltpu.make_async_copy(gf_hbm, gf_ref, sem_p.at[1]),
             pltpu.make_async_copy(len_hbm, lens, sem_p.at[2])]
    for cp in x_in + small:
        cp.start()
    for cp in x_in:
        cp.wait()
    for i in range(3):
        wq_copy(0, i).start()
    pl.semaphore_wait(barrier, 3)
    for cp in x_out:
        cp.start()
    for cp in small + x_out:
        cp.wait()

    def norm_rows(piece, gain):
        scales = []
        for r in range(2 * rows // 16):
            a, b = (piece(k, r * 16).astype(F32) for k in range(2))
            ms = jnp.sum(a * a + b * b, axis=-1, keepdims=True) * (1.0 / d)
            scales.append(lax.rsqrt(ms + NORM_EPS))
        for r in range(2 * rows // 16):
            for k in range(2):
                hbuf[pl.ds(r * 16, 16), pl.ds(k * half, half)] = (
                    piece(k, r * 16).astype(F32) * scales[r] * gain[:, k * half:(k + 1) * half]).astype(BF)

    def layer_body(l, carry):
        norm_rows(lambda k, r: xfull[k, pl.ds(r, 16), :], ga_ref[pl.ds(l, 1), :])
        q_sends = []
        for i, (h0, nh) in enumerate(qsplit):
            wq_copy(l, i).wait()

            @pl.when(l == 0)
            def _():
                if i == 0:
                    for g in range(n_grp):
                        c_copy(0, g).start()
                else:
                    for nb in range((i - 1) * n_ob // 2, i * n_ob // 2):
                        wo_copy(0, nb).start()

            acc = jnp.dot(hbuf[...], r1[:, h0 * kv:(h0 + nh) * kv], preferred_element_type=F32)
            acc = acc.astype(BF).astype(F32)
            base = pl.multiple_of((c * (heads // 2) + h0) * rows, rows)
            for hh in range(0, nh, 2):
                two = acc[:, hh * kv:(hh + 2) * kv]
                rolled = pltpu.roll(two, kv, 1)
                for t in range(n_lt):
                    lanes = slice(t * 128, (t + 1) * 128)
                    q3[t, pl.ds(base + hh * rows, rows), :] = two[:rows, lanes]
                    q3[t, pl.ds(base + (hh + 1) * rows, rows), :] = rolled[:rows, lanes]
                    qs[t, pl.ds((h0 + hh) * rows, rows), :] = two[rows:, lanes]
                    qs[t, pl.ds((h0 + hh + 1) * rows, rows), :] = rolled[rows:, lanes]
            cp = rc(qs.at[:, pl.ds(h0 * rows, nh * rows)], q3.at[:, pl.ds(base, nh * rows)], q_s.at[i], q_r.at[i],
                    partner)
            cp.start()
            q_sends.append(cp)
        for cp in ffn_copies(l):
            cp.start()
        for cp in q_sends:
            cp.wait()

        def o_copy(g):
            src = oall.at[:, pl.ds(pl.multiple_of(g * GRP, GRP), GRP)]
            dst = oall.at[:, pl.ds(pl.multiple_of(rows + g * GRP, GRP), GRP)]
            return rc(src, dst, o_s.at[g], o_r.at[g], partner)

        pos = lax.broadcasted_iota(jnp.int32, (heads, seq), 1)
        first = lax.rem(lax.broadcasted_iota(jnp.int32, (GRP * heads, seq), 0), 2 * heads) < heads

        def scores(g, b):
            row = g * GRP + b
            qb = jnp.concatenate(
                [jnp.concatenate([q3[t, pl.ds(row + k, heads, stride=rows), :] for t in range(n_lt)], axis=1)
                 for k in range(2)], axis=0)
            keys = jnp.concatenate([r3[row], r3[row + 1]], axis=1)
            s = jnp.dot(qb[:, :kv].astype(BF), keys, preferred_element_type=F32) * scale
            sbuf[g % 2, pl.ds(b * heads, heads), :] = jnp.where(pos < lens[row], s[:heads, :seq], -jnp.inf)
            sbuf[g % 2, pl.ds((b + 1) * heads, heads), :] = jnp.where(pos < lens[row + 1], s[heads:, seq:], -jnp.inf)

        def mix(g, b):
            row = g * GRP + b
            vals = jnp.concatenate([r3[row, 0:latent, :], r3[row + 1, 0:latent, :]], axis=1)
            o = lax.dot_general(pbuf[pl.ds(b * heads, 2 * heads), :], vals, (((1,), (1,)), ((), ())),
                                preferred_element_type=F32)
            for t in range(latent // 128):
                o3[t, pl.ds(b, heads, stride=GRP), :] = o[:heads, t * 128:(t + 1) * 128]
                o3[t, pl.ds(b + 1, heads, stride=GRP), :] = o[heads:, t * 128:(t + 1) * 128]

        c_copy(l, 0).wait()
        for b in range(0, GRP, 2):
            scores(0, b)
        for g in range(n_grp):
            if g + 1 < n_grp:
                c_copy(l, g + 1).wait()
            s = sbuf[g % 2]
            e = jnp.exp(s - jnp.max(s, axis=-1, keepdims=True))
            p = e / jnp.sum(e, axis=-1, keepdims=True)
            pbuf[:, :seq] = jnp.where(first, p, 0.0).astype(BF)
            pbuf[:, seq:] = jnp.where(first, 0.0, p).astype(BF)
            for b in range(0, GRP, 2):
                if g + 1 < n_grp:
                    scores(g + 1, b)
                mix(g, b)
            for t in range(latent // 128):
                oall[:, pl.ds(g * GRP, GRP), t * 128:(t + 1) * 128] = o3[t].astype(BF).reshape(heads, GRP, 128)
            o_copy(g).start()
        for g in range(n_grp):
            o_copy(g).wait()

        @pl.when(l + 1 < layers)
        def _():
            for g in range(n_grp):
                c_copy(l + 1, g).start()

        pa, pb = pl.ds(0, rows), pl.ds(rows, rows)

        def ag(k, ch, part, dev, hx=None):
            hx = c if hx is None else hx
            ref = xg.at[ch, hx] if part is None else xg.at[ch, hx, part]
            return rc(ref, ref, ag_s.at[k], ag_r.at[k], dev)

        def ag_first(nb, ch, part, dev):
            ref = xg.at[ch, c, part, pl.ds(pl.multiple_of(nb * OBLK, OBLK), OBLK)]
            k = nb if part is pa else n_ob + nb
            return rc(ref, ref, af_s.at[k], af_r.at[k], dev)

        sends = [ag(4, chip, None, partner), ag(5, chip, pb, right), ag(6, chip, pa, left)]
        fwd = [ag(7, ch_l, pa, right), ag(8, ch_r, pb, left), ag(9, ch_l, pa, partner), ag(10, ch_r, pb, partner),
               ag(11, ch_l, pb, partner), ag(12, ch_r, pa, partner), ag(13, ch_o, pa, partner),
               ag(14, ch_o, pb, partner)]

        def got(k, ch, part, hx=None):
            ag(k, ch, part, partner, hx).wait_recv()

        def out_block(nb, carry):
            wo_copy(l, nb).wait()
            cols = pl.ds(pl.multiple_of(nb * OBLK, OBLK), OBLK)
            acc = jnp.dot(oall[0], r2[nb, 0:latent, :], preferred_element_type=F32)
            for h in range(1, heads):
                acc = acc + jnp.dot(oall[h], r2[nb, h * latent:(h + 1) * latent, :], preferred_element_type=F32)
            xn = (xfull[c, :, cols].astype(F32) + acc).astype(BF)
            xg[chip, c, pl.ds(pl.multiple_of(c * rows, rows), rows), cols] = xn[:rows]
            xg[chip, c, pl.ds(pl.multiple_of((1 - c) * rows, rows), rows), cols] = xn[rows:]
            ag_first(nb, chip, pa, right).start()
            ag_first(nb, chip, pb, left).start()
            return carry

        lax.fori_loop(0, n_ob, out_block, 0)
        for cp in (sends[1], sends[2], sends[0]):
            cp.start()

        @pl.when(l + 1 < layers)
        def _():
            for nb in range(n_ob):
                wo_copy(l + 1, nb).start()

        hr = rows // 2

        def rs_sub(slot, dst, base, sub, k, dev):
            return rc(sown.at[slot, pl.ds(base + sub * hr, hr)], rb.at[dst, pl.ds(sub * hr, hr)],
                      rs_s.at[k], rs_r.at[k], dev)

        unm = [rc(sown.at[0, pa], rb.at[0], rs_s.at[0], rs_r.at[0], left),
               rc(sown.at[0, pb], rb.at[1], rs_s.at[1], rs_r.at[1], right)]
        rly = [rs_sub(1, 2, 0, 0, 2, right), rs_sub(1, 3, rows, 0, 3, left),
               rs_sub(1, 2, 0, 1, 4, right), rs_sub(1, 3, rows, 1, 5, left)]
        mrg = [rs_sub(2, 4, 0, 0, 6, right), rs_sub(2, 5, rows, 0, 7, left),
               rs_sub(2, 4, 0, 1, 8, right), rs_sub(2, 5, rows, 1, 9, left)]

        hc = half // 2

        def pd_copy(i, hf):
            cols = pl.ds(hf * hc, hc)
            return rc(pst.at[lax.rem(i, 2), :, cols], prd.at[i, :, cols], pd_s.at[2 * i + hf], pd_r.at[2 * i + hf],
                      partner)

        def pair_sum(i):
            for hf in range(2):
                pd_copy(i, hf).wait_recv()
            sown[i] = sown[i] + prd[i]

        for cp in ffn_copies(l):
            cp.wait()

        def chunk(i, carry):
            p0 = lax.rem(chip + chips - 1 - i, chips)
            p1 = lax.rem(chip + 1 + i, chips)

            @pl.when(i == 0)
            def _():
                for nb in range(n_ob):
                    ag_first(nb, ch_l, pa, right).wait_recv()
                fwd[0].start()
                fwd[2].start()
                for nb in range(n_ob):
                    ag_first(nb, ch_r, pb, left).wait_recv()
                fwd[1].start()
                fwd[3].start()
                got(9, ch_l, pa, 1 - c)
                got(10, ch_r, pb, 1 - c)

            @pl.when(i == 1)
            def _():
                pair_sum(0)
                unm[0].start()
                unm[1].start()
                got(7, ch_o, pa)
                fwd[6].start()
                got(8, ch_o, pb)
                fwd[7].start()
                got(13, ch_o, pa, 1 - c)
                got(14, ch_o, pb, 1 - c)

            @pl.when(i == 2)
            def _():
                pair_sum(1)
                for cp in rly:
                    cp.start()
                got(11, ch_l, pb, 1 - c)
                got(12, ch_r, pa, 1 - c)

            @pl.when(i == 3)
            def _():
                got(4, chip, None, 1 - c)

            norm_rows(lambda h, r: xg[p0 if r < rows else p1, h, pl.ds(r, 16), :], gf_ref[pl.ds(l, 1), :])
            for lo in range(0, ff, 512):
                w = min(512, ff - lo)
                gate = jnp.dot(hbuf[...], r1[:, lo:lo + w], preferred_element_type=F32)
                up = jnp.dot(hbuf[...], r1[:, ff + lo:ff + lo + w], preferred_element_type=F32)
                hid[:, lo:lo + w] = (jax.nn.silu(gate) * up).astype(BF)

            @pl.when(i == 0)
            def _():
                got(5, ch_l, pb)
                fwd[4].start()
                got(6, ch_r, pa)
                fwd[5].start()

            @pl.when(i == 3)
            def _():
                pair_sum(2)

            @pl.when(i >= 2)
            def _():
                for hf in range(2):
                    pd_copy(i - 2, hf).wait_send()

            slot = lax.rem(i, 2)
            for hf in range(2):
                pst[slot, :, hf * hc:(hf + 1) * hc] = jnp.dot(
                    hid[...], r1[0:ff, 2 * ff + hf * hc:2 * ff + (hf + 1) * hc], preferred_element_type=F32)
                pd_copy(i, hf).start()
            for hf in range(2):
                lo = 2 * ff + half + hf * hc
                sown[i, :, hf * hc:(hf + 1) * hc] = jnp.dot(hid[...], r1[0:ff, lo:lo + hc], preferred_element_type=F32)
            return carry

        lax.fori_loop(0, chips, chunk, 0)

        @pl.when(l + 1 < layers)
        def _():
            for i in range(3):
                wq_copy(l + 1, i).start()

        for cp in sends + fwd:
            cp.wait_send()
        for nb in range(n_ob):
            ag_first(nb, chip, pa, right).wait_send()
            ag_first(nb, chip, pb, left).wait_send()
        for i in range(4):
            sub = pl.ds((i // 2) * hr, hr)
            dst = pl.ds((i % 2) * rows + (i // 2) * hr, hr)
            rly[i].wait_recv()
            sown[2, dst] = sown[2, dst] + rb[2 + i % 2, sub]
            mrg[i].start()
        for i in (2, 3):
            for hf in range(2):
                pd_copy(i, hf).wait_send()
        pair_sum(3)
        unm[0].wait_recv()
        unm[1].wait_recv()
        rb[0] = rb[0] + sown[3, pa] + xg[chip, c, pa].astype(F32)
        rb[1] = rb[1] + sown[3, pb] + xg[chip, c, pb].astype(F32)
        for cp in mrg:
            cp.wait_recv()
        xfull[c, pl.ds(0, rows)] = (rb[c] + rb[4 + c]).astype(BF)
        xfull[c, pl.ds(rows, rows)] = (rb[1 - c] + rb[5 - c]).astype(BF)
        xx = [rc(xfull.at[c, pl.ds(rows, rows)], xfull.at[c, pl.ds(0, rows)], xx_s.at[0], xx_r.at[0], partner),
              rc(xfull.at[c, pl.ds(0, rows)], xfull.at[c, pl.ds(rows, rows)], xx_s.at[1], xx_r.at[1], partner)]
        for cp in xx:
            cp.start()
        for cp in unm + rly + mrg:
            cp.wait_send()
        for cp in xx:
            cp.wait()
        return carry

    lax.fori_loop(0, layers, layer_body, 0)
    x_fin = [pltpu.make_async_copy(xfull.at[k, pl.ds(0, rows)], out_hbm.at[:, pl.ds(k * half, half)], sem_x.at[k])
             for k in range(2)]
    for cp in x_fin:
        cp.start()
    for cp in x_fin:
        cp.wait()


def solution(mesh):
    row_axes = ('replica', 'dp')
    n = mesh.shape['dp']
    chips = n // 2

    def local_step(x_rows, len_rows, cache, attn_gain, ffn_gain, w_query, w_attn_out, w_up, w_gate, w_down):
        layers, rows, seq, kv = cache.shape
        d = x_rows.shape[1]
        heads = w_query.shape[2] // kv
        latent = w_attn_out.shape[1] // heads
        ff = w_up.shape[2]
        half = d // 2
        qh = heads * kv // 2
        dims = (layers, rows, seq, kv, heads, latent, d, ff, chips)
        n_grp = rows // GRP
        n_ob = half // OBLK
        n_lt = pl.cdiv(kv, 128)
        any_spec = pl.BlockSpec(memory_space=pl.ANY)
        dma = pltpu.SemaphoreType.DMA
        return pl.pallas_call(
            functools.partial(kernel, dims),
            out_shape=jax.ShapeDtypeStruct(x_rows.shape, x_rows.dtype),
            in_specs=[any_spec] * 10,
            out_specs=any_spec,
            scratch_shapes=[
                pltpu.SMEM((rows,), jnp.int32),
                pltpu.VMEM(attn_gain.shape, F32),
                pltpu.VMEM(ffn_gain.shape, F32),
                pltpu.VMEM((d, max(qh, 2 * ff + d)), BF),
                pltpu.VMEM((n_ob, heads * latent, OBLK), BF),
                pltpu.VMEM((rows, kv, seq), BF),
                pltpu.VMEM((2, 2 * rows, half), BF),
                pltpu.VMEM((2 * rows, d), BF),
                pltpu.VMEM((n_lt, heads * rows, 128), F32),
                pltpu.VMEM((n_lt, heads // 2 * rows, 128), F32),
                pltpu.VMEM((2, GRP * heads, seq), F32),
                pltpu.VMEM((GRP * heads, 2 * seq), BF),
                pltpu.VMEM((latent // 128, GRP * heads, 128), F32),
                pltpu.VMEM((heads, 2 * rows, latent), BF),
                pltpu.VMEM((chips, 2, 2 * rows, half), BF),
                pltpu.VMEM((chips, 2 * rows, half), F32),
                pltpu.VMEM((chips, 2 * rows, half), F32),
                pltpu.VMEM((2, 2 * rows, half), F32),
                pltpu.VMEM((2 * rows, ff), BF),
                pltpu.VMEM((6, rows, half), F32),
                dma((3,)), dma((4,)), dma((n_grp,)), dma((n_ob,)), dma((4,)), dma((2,)),
                dma((2,)), dma((2,)), dma((4,)), dma((4,)), dma((n_grp,)), dma((n_grp,)),
                dma((2 * n_ob,)), dma((2 * n_ob,)), dma((15,)), dma((15,)), dma((2 * chips,)), dma((2 * chips,)), dma((10,)), dma((10,)),
                dma((2,)), dma((2,)),
            ],
            compiler_params=pltpu.CompilerParams(
                collective_id=0, has_side_effects=True, vmem_limit_bytes=67043328),
        )(x_rows, len_rows, jnp.swapaxes(cache, 2, 3), attn_gain, ffn_gain, w_query, w_attn_out, w_up, w_gate, w_down)

    return jax.shard_map(
        local_step,
        mesh=mesh,
        in_specs=(P(row_axes, None), P(row_axes), P(None, row_axes, None, None), P(), P(), P(), P(),
                  P(None, None, 'dp'), P(None, None, 'dp'), P(None, 'dp', None)),
        out_specs=P(row_axes, None),
        check_vma=False,
    )
```

```python
import functools

import jax
import jax.numpy as jnp
from jax import lax
from jax.experimental import pallas as pl
from jax.experimental.pallas import tpu as pltpu
from jax.sharding import PartitionSpec as P

NORM_EPS = 1e-6
BF = jnp.bfloat16
F32 = jnp.float32
GRP = 16
OBLK = 512


def kernel(dims, x_hbm, len_hbm, cache_hbm, ga_hbm, gf_hbm, wq_hbm, wo_hbm, wu_hbm, wg_hbm, wd_hbm, out_hbm,
           lens, ga_ref, gf_ref, r1, r2, r3, xfull, hbuf, q3, qs, sbuf, pbuf, o3, oall, xg, sown, prd, pst, hid, rb,
           sem_p, sem_w, sem_c, sem_o, sem_f, sem_x, xi_s, xi_r, q_s, q_r, o_s, o_r, af_s, af_r, ag_s, ag_r, pd_s, pd_r, rs_s, rs_r,
           xx_s, xx_r):
    layers, rows, seq, kv, heads, latent, d, ff, chips = dims
    half = d // 2
    hc = half // 2
    qh = heads * kv // 2
    qsplit = ((0, heads // 4), (heads // 4, heads // 8), (3 * heads // 8, heads // 8))
    scale = (3 * (kv - latent)) ** -0.5
    n_grp = rows // GRP
    n_ob = half // OBLK
    n_lt = pl.cdiv(kv, 128)

    me = lax.axis_index('dp')
    c = lax.rem(me, 2)
    chip = me // 2
    partner = me + 1 - 2 * c
    right = lax.rem(chip + 1, chips) * 2 + c
    left = lax.rem(chip + chips - 1, chips) * 2 + c
    ch_r = lax.rem(chip + 1, chips)
    ch_l = lax.rem(chip + chips - 1, chips)
    ch_o = lax.rem(chip + 2, chips)

    def rc(src, dst, ss, rs, dev):
        return pltpu.make_async_remote_copy(src_ref=src, dst_ref=dst, send_sem=ss, recv_sem=rs,
                                            device_id={'dp': dev}, device_id_type=pl.DeviceIdType.MESH)

    def wq_copy(l, i):
        lo, w = qsplit[i][0] * kv, qsplit[i][1] * kv
        cols = pl.ds(pl.multiple_of(c * qh + lo, 128), w)
        return pltpu.make_async_copy(wq_hbm.at[l, :, cols], r1.at[:, pl.ds(lo, w)], sem_w.at[i])

    def c_copy(l, g):
        rs = pl.ds(pl.multiple_of(g * GRP, GRP), GRP)
        return pltpu.make_async_copy(cache_hbm.at[l, rs], r3.at[rs], sem_c.at[g])

    def wo_copy(l, nb):
        cols = pl.ds(pl.multiple_of(c * half + nb * OBLK, 128), OBLK)
        return pltpu.make_async_copy(wo_hbm.at[l, :, cols], r2.at[nb], sem_o.at[nb])

    def ffn_copies(l):
        lo = pl.ds(pl.multiple_of((1 - c) * half, 128), half)
        hi = pl.ds(pl.multiple_of(c * half, 128), half)
        return (
            pltpu.make_async_copy(wg_hbm.at[l], r1.at[:, pl.ds(0, ff)], sem_f.at[0]),
            pltpu.make_async_copy(wu_hbm.at[l], r1.at[:, pl.ds(ff, ff)], sem_f.at[1]),
            pltpu.make_async_copy(wd_hbm.at[l, :, lo], r1.at[pl.ds(0, ff), pl.ds(2 * ff, half)], sem_f.at[2]),
            pltpu.make_async_copy(wd_hbm.at[l, :, hi], r1.at[pl.ds(0, ff), pl.ds(2 * ff + half, half)], sem_f.at[3]),
        )

    barrier = pltpu.get_barrier_semaphore()
    for dev in (partner, left, right):
        pl.semaphore_signal(barrier, inc=1, device_id={'dp': dev}, device_id_type=pl.DeviceIdType.MESH)
    x_in = [pltpu.make_async_copy(x_hbm.at[:, pl.ds(k * hc, hc)], xfull.at[k, pl.ds(0, rows)], sem_x.at[k])
            for k in range(4)]
    x_out = [rc(xfull.at[:, pl.ds(0, rows)], xfull.at[:, pl.ds(rows, rows)], xi_s.at[0], xi_r.at[0], partner)]
    small = [pltpu.make_async_copy(ga_hbm, ga_ref, sem_p.at[0]), pltpu.make_async_copy(gf_hbm, gf_ref, sem_p.at[1]),
             pltpu.make_async_copy(len_hbm, lens, sem_p.at[2])]
    for cp in x_in + small:
        cp.start()
    for cp in x_in:
        cp.wait()
    for i in range(3):
        wq_copy(0, i).start()
    pl.semaphore_wait(barrier, 3)
    for cp in x_out:
        cp.start()
    for cp in small + x_out:
        cp.wait()

    def norm_rows(piece, gain):
        scales = []
        for r in range(2 * rows // 16):
            sq = [piece(k, r * 16).astype(F32) for k in range(4)]
            ms = jnp.sum(sum(a * a for a in sq), axis=-1, keepdims=True) * (1.0 / d)
            scales.append(lax.rsqrt(ms + NORM_EPS))
        for r in range(2 * rows // 16):
            for k in range(4):
                hbuf[pl.ds(r * 16, 16), pl.ds(k * hc, hc)] = (
                    piece(k, r * 16).astype(F32) * scales[r] * gain[:, k * hc:(k + 1) * hc]).astype(BF)

    def layer_body(l, carry):
        norm_rows(lambda k, r: xfull[k, pl.ds(r, 16), :], ga_ref[pl.ds(l, 1), :])
        q_sends = []
        for i, (h0, nh) in enumerate(qsplit):
            wq_copy(l, i).wait()

            @pl.when(l == 0)
            def _():
                if i == 0:
                    for g in range(n_grp):
                        c_copy(0, g).start()
                else:
                    for nb in range((i - 1) * n_ob // 2, i * n_ob // 2):
                        wo_copy(0, nb).start()

            acc = jnp.dot(hbuf[...], r1[:, h0 * kv:(h0 + nh) * kv], preferred_element_type=F32)
            acc = acc.astype(BF).astype(F32)
            base = pl.multiple_of((c * (heads // 2) + h0) * rows, rows)
            for hh in range(0, nh, 2):
                two = acc[:, hh * kv:(hh + 2) * kv]
                rolled = pltpu.roll(two, kv, 1)
                for t in range(n_lt):
                    lanes = slice(t * 128, (t + 1) * 128)
                    q3[t, pl.ds(base + hh * rows, rows), :] = two[:rows, lanes]
                    q3[t, pl.ds(base + (hh + 1) * rows, rows), :] = rolled[:rows, lanes]
                    qs[t, pl.ds((h0 + hh) * rows, rows), :] = two[rows:, lanes]
                    qs[t, pl.ds((h0 + hh + 1) * rows, rows), :] = rolled[rows:, lanes]
            cp = rc(qs.at[:, pl.ds(h0 * rows, nh * rows)], q3.at[:, pl.ds(base, nh * rows)], q_s.at[i], q_r.at[i],
                    partner)
            cp.start()
            q_sends.append(cp)
        for cp in ffn_copies(l):
            cp.start()
        for cp in q_sends:
            cp.wait()

        def o_copy(g):
            src = oall.at[:, pl.ds(pl.multiple_of(g * GRP, GRP), GRP)]
            dst = oall.at[:, pl.ds(pl.multiple_of(rows + g * GRP, GRP), GRP)]
            return rc(src, dst, o_s.at[g], o_r.at[g], partner)

        pos = lax.broadcasted_iota(jnp.int32, (heads, seq), 1)
        first = lax.rem(lax.broadcasted_iota(jnp.int32, (GRP * heads, seq), 0), 2 * heads) < heads

        def scores(g, b):
            row = g * GRP + b
            qb = jnp.concatenate(
                [jnp.concatenate([q3[t, pl.ds(row + k, heads, stride=rows), :] for t in range(n_lt)], axis=1)
                 for k in range(2)], axis=0)
            keys = jnp.concatenate([r3[row], r3[row + 1]], axis=1)
            s = jnp.dot(qb[:, :kv].astype(BF), keys, preferred_element_type=F32) * scale
            sbuf[g % 2, pl.ds(b * heads, heads), :] = jnp.where(pos < lens[row], s[:heads, :seq], -jnp.inf)
            sbuf[g % 2, pl.ds((b + 1) * heads, heads), :] = jnp.where(pos < lens[row + 1], s[heads:, seq:], -jnp.inf)

        def mix(g, b):
            row = g * GRP + b
            vals = jnp.concatenate([r3[row, 0:latent, :], r3[row + 1, 0:latent, :]], axis=1)
            o = lax.dot_general(pbuf[g % 2, pl.ds(b * heads, 2 * heads), :], vals, (((1,), (1,)), ((), ())),
                                preferred_element_type=F32)
            for t in range(latent // 128):
                o3[t, pl.ds(b, heads, stride=GRP), :] = o[:heads, t * 128:(t + 1) * 128]
                o3[t, pl.ds(b + 1, heads, stride=GRP), :] = o[heads:, t * 128:(t + 1) * 128]

        def softmax(g):
            s = sbuf[g % 2]
            e = jnp.exp(s - jnp.max(s, axis=-1, keepdims=True))
            p = e / jnp.sum(e, axis=-1, keepdims=True)
            pbuf[g % 2, :, :seq] = jnp.where(first, p, 0.0).astype(BF)
            pbuf[g % 2, :, seq:] = jnp.where(first, 0.0, p).astype(BF)

        for gs in range(n_grp + 2):
            gx = gs - 2
            if gs < n_grp:
                c_copy(l, gs).wait()
            if 0 < gs <= n_grp:
                softmax(gs - 1)
            for b in range(0, GRP, 2):
                if gs < n_grp:
                    scores(gs, b)
                if gx >= 0:
                    mix(gx, b)
            if gx >= 0:
                for t in range(latent // 128):
                    oall[:, pl.ds(gx * GRP, GRP), t * 128:(t + 1) * 128] = o3[t].astype(BF).reshape(heads, GRP, 128)
                o_copy(gx).start()
        for g in range(n_grp):
            o_copy(g).wait()

        @pl.when(l + 1 < layers)
        def _():
            for g in range(n_grp):
                c_copy(l + 1, g).start()

        pa, pb = pl.ds(0, rows), pl.ds(rows, rows)

        def ag(k, ch, part, dev, hx=None):
            hx = c if hx is None else hx
            quarters = pl.ds(2 * hx, 2)
            ref = xg.at[ch, quarters] if part is None else xg.at[ch, quarters, part]
            return rc(ref, ref, ag_s.at[k], ag_r.at[k], dev)

        def ag_first(hf, ch, part, dev):
            ref = xg.at[ch, 2 * c + hf, part]
            k = hf if part is pa else 2 + hf
            return rc(ref, ref, af_s.at[k], af_r.at[k], dev)

        sends = [ag(4, chip, None, partner), ag(5, chip, pb, right), ag(6, chip, pa, left)]
        fwd = [ag(7, ch_l, pa, right), ag(8, ch_r, pb, left), ag(9, ch_l, pa, partner), ag(10, ch_r, pb, partner),
               ag(11, ch_l, pb, partner), ag(12, ch_r, pa, partner), ag(13, ch_o, pa, partner),
               ag(14, ch_o, pb, partner)]

        def got(k, ch, part, hx=None):
            ag(k, ch, part, partner, hx).wait_recv()

        def out_block(nb, carry):
            wo_copy(l, nb).wait()
            per = hc // OBLK
            cols = pl.ds(pl.multiple_of(lax.rem(nb, per) * OBLK, OBLK), OBLK)
            acc = jnp.dot(oall[0], r2[nb, 0:latent, :], preferred_element_type=F32)
            for h in range(1, heads):
                acc = acc + jnp.dot(oall[h], r2[nb, h * latent:(h + 1) * latent, :], preferred_element_type=F32)
            quarter = 2 * c + nb // per
            xn = (xfull[quarter, :, cols].astype(F32) + acc).astype(BF)
            xg[chip, quarter, pl.ds(pl.multiple_of(c * rows, rows), rows), cols] = xn[:rows]
            xg[chip, quarter, pl.ds(pl.multiple_of((1 - c) * rows, rows), rows), cols] = xn[rows:]

            @pl.when(nb == per - 1)
            def _():
                ag_first(0, chip, pa, right).start()
                ag_first(0, chip, pb, left).start()
            return carry

        lax.fori_loop(0, n_ob, out_block, 0)
        for cp in (ag_first(1, chip, pa, right), ag_first(1, chip, pb, left), sends[0], sends[1], sends[2]):
            cp.start()

        @pl.when(l + 1 < layers)
        def _():
            for nb in range(n_ob):
                wo_copy(l + 1, nb).start()

        def rs(group, slot, hf, way):
            part, dev = ((pa, right), (pb, left))[way]
            if group == 0:
                dev = (left, right)[way]
            k = group * 4 + hf * 2 + way
            return rc(sown.at[slot, hf, part], rb.at[2 * group + way, hf], rs_s.at[k], rs_r.at[k], dev)

        unm = [[rs(0, 1, hf, way) for way in range(2)] for hf in range(2)]
        rly = [[rs(1, 2, hf, way) for way in range(2)] for hf in range(2)]
        mrg = [[rs(2, 3, hf, way) for way in range(2)] for hf in range(2)]

        def pd_copy(i, hf):
            return rc(pst.at[lax.rem(i, 2), hf], prd.at[i, hf], pd_s.at[2 * i + hf], pd_r.at[2 * i + hf], partner)

        def pair_sum(i, hf):
            pd_copy(i, hf).wait_recv()
            sown[i, hf] = sown[i, hf] + prd[i, hf]

        for cp in ffn_copies(l):
            cp.wait()

        def chunk(i, carry):
            p0 = lax.rem(chip + chips - i, chips)
            p1 = lax.rem(chip + i, chips)

            @pl.when(i == 0)
            def _():
                got(4, chip, None, 1 - c)

            @pl.when(i == 1)
            def _():
                for hf in range(2):
                    ag_first(hf, ch_l, pa, right).wait_recv()
                fwd[0].start()
                fwd[2].start()
                for hf in range(2):
                    ag_first(hf, ch_r, pb, left).wait_recv()
                fwd[1].start()
                fwd[3].start()
                got(9, ch_l, pa, 1 - c)
                got(10, ch_r, pb, 1 - c)

            @pl.when(i == 2)
            def _():
                for hf in range(2):
                    pair_sum(1, hf)
                    for cp in unm[hf]:
                        cp.start()
                got(5, ch_l, pb)
                fwd[4].start()
                got(6, ch_r, pa)
                fwd[5].start()
                got(7, ch_o, pa)
                fwd[6].start()
                got(8, ch_o, pb)
                fwd[7].start()
                got(13, ch_o, pa, 1 - c)
                got(14, ch_o, pb, 1 - c)

            @pl.when(i == 3)
            def _():
                for hf in range(2):
                    pair_sum(2, hf)
                    for cp in rly[hf]:
                        cp.start()
                got(11, ch_l, pb, 1 - c)
                got(12, ch_r, pa, 1 - c)

            norm_rows(lambda q, r: xg[p0 if r < rows else p1, q, pl.ds(r, 16), :], gf_ref[pl.ds(l, 1), :])
            for lo in range(0, ff, 512):
                w = min(512, ff - lo)
                gate = jnp.dot(hbuf[...], r1[:, lo:lo + w], preferred_element_type=F32)
                up = jnp.dot(hbuf[...], r1[:, ff + lo:ff + lo + w], preferred_element_type=F32)
                hid[:, lo:lo + w] = (jax.nn.silu(gate) * up).astype(BF)

            @pl.when(i == 2)
            def _():
                for hf in range(2):
                    pair_sum(0, hf)

            @pl.when(i >= 2)
            def _():
                for hf in range(2):
                    pd_copy(i - 2, hf).wait_send()

            slot = lax.rem(i, 2)
            for hf in range(2):
                pst[slot, hf] = jnp.dot(
                    hid[...], r1[0:ff, 2 * ff + hf * hc:2 * ff + (hf + 1) * hc], preferred_element_type=F32)
                pd_copy(i, hf).start()
            for hf in range(2):
                lo = 2 * ff + half + hf * hc
                sown[i, hf] = jnp.dot(hid[...], r1[0:ff, lo:lo + hc], preferred_element_type=F32)
            return carry

        lax.fori_loop(0, chips, chunk, 0)

        @pl.when(l + 1 < layers)
        def _():
            for i in range(3):
                wq_copy(l + 1, i).start()

        for cp in sends + fwd:
            cp.wait_send()
        for hf in range(2):
            ag_first(hf, chip, pa, right).wait_send()
            ag_first(hf, chip, pb, left).wait_send()
        for hf in range(2):
            pair_sum(3, hf)
            for way, part in enumerate((pa, pb)):
                rly[hf][way].wait_recv()
                sown[3, hf, part] = sown[3, hf, part] + rb[2 + way, hf]
                mrg[hf][way].start()
        for i in (2, 3):
            for hf in range(2):
                pd_copy(i, hf).wait_send()
        for hf in range(2):
            for way, part in enumerate((pa, pb)):
                unm[hf][way].wait_recv()
                rb[way, hf] = rb[way, hf] + sown[0, hf, part] + xg[chip, 2 * c + hf, part].astype(F32)
        own, oth = pl.ds(0, rows), pl.ds(rows, rows)
        xx = []
        for hf in range(2):
            for way in range(2):
                mrg[hf][way].wait_recv()
            ref = xfull.at[2 * c + hf]
            xfull[2 * c + hf, own] = (rb[c, hf] + rb[4 + c, hf]).astype(BF)
            xfull[2 * c + hf, oth] = (rb[1 - c, hf] + rb[5 - c, hf]).astype(BF)
            for k, (a, b) in enumerate(((oth, own), (own, oth))):
                cp = rc(ref.at[a], ref.at[b], xx_s.at[2 * hf + k], xx_r.at[2 * hf + k], partner)
                cp.start()
                xx.append(cp)
        for group in (unm, rly, mrg):
            for hf in range(2):
                for cp in group[hf]:
                    cp.wait_send()
        for cp in xx:
            cp.wait()
        return carry

    lax.fori_loop(0, layers, layer_body, 0)
    x_fin = [pltpu.make_async_copy(xfull.at[k, pl.ds(0, rows)], out_hbm.at[:, pl.ds(k * hc, hc)], sem_x.at[k])
             for k in range(4)]
    for cp in x_fin:
        cp.start()
    for cp in x_fin:
        cp.wait()


def solution(mesh):
    row_axes = ('replica', 'dp')
    n = mesh.shape['dp']
    chips = n // 2

    def local_step(x_rows, len_rows, cache, attn_gain, ffn_gain, w_query, w_attn_out, w_up, w_gate, w_down):
        layers, rows, seq, kv = cache.shape
        d = x_rows.shape[1]
        heads = w_query.shape[2] // kv
        latent = w_attn_out.shape[1] // heads
        ff = w_up.shape[2]
        half = d // 2
        qh = heads * kv // 2
        dims = (layers, rows, seq, kv, heads, latent, d, ff, chips)
        n_grp = rows // GRP
        n_ob = half // OBLK
        n_lt = pl.cdiv(kv, 128)
        any_spec = pl.BlockSpec(memory_space=pl.ANY)
        dma = pltpu.SemaphoreType.DMA
        return pl.pallas_call(
            functools.partial(kernel, dims),
            out_shape=jax.ShapeDtypeStruct(x_rows.shape, x_rows.dtype),
            in_specs=[any_spec] * 10,
            out_specs=any_spec,
            scratch_shapes=[
                pltpu.SMEM((rows,), jnp.int32),
                pltpu.VMEM(attn_gain.shape, F32),
                pltpu.VMEM(ffn_gain.shape, F32),
                pltpu.VMEM((d, max(qh, 2 * ff + d)), BF),
                pltpu.VMEM((n_ob, heads * latent, OBLK), BF),
                pltpu.VMEM((rows, kv, seq), BF),
                pltpu.VMEM((4, 2 * rows, half // 2), BF),
                pltpu.VMEM((2 * rows, d), BF),
                pltpu.VMEM((n_lt, heads * rows, 128), F32),
                pltpu.VMEM((n_lt, heads // 2 * rows, 128), F32),
                pltpu.VMEM((2, GRP * heads, seq), F32),
                pltpu.VMEM((2, GRP * heads, 2 * seq), BF),
                pltpu.VMEM((latent // 128, GRP * heads, 128), F32),
                pltpu.VMEM((heads, 2 * rows, latent), BF),
                pltpu.VMEM((chips, 4, 2 * rows, half // 2), BF),
                pltpu.VMEM((chips, 2, 2 * rows, half // 2), F32),
                pltpu.VMEM((chips, 2, 2 * rows, half // 2), F32),
                pltpu.VMEM((2, 2, 2 * rows, half // 2), F32),
                pltpu.VMEM((2 * rows, ff), BF),
                pltpu.VMEM((6, 2, rows, half // 2), F32),
                dma((3,)), dma((4,)), dma((n_grp,)), dma((n_ob,)), dma((4,)), dma((4,)),
                dma((2,)), dma((2,)), dma((4,)), dma((4,)), dma((n_grp,)), dma((n_grp,)),
                dma((4,)), dma((4,)), dma((15,)), dma((15,)), dma((2 * chips,)), dma((2 * chips,)), dma((12,)), dma((12,)),
                dma((4,)), dma((4,)),
            ],
            compiler_params=pltpu.CompilerParams(
                collective_id=0, has_side_effects=True, vmem_limit_bytes=67043328),
        )(x_rows, len_rows, jnp.swapaxes(cache, 2, 3), attn_gain, ffn_gain, w_query, w_attn_out, w_up, w_gate, w_down)

    return jax.shard_map(
        local_step,
        mesh=mesh,
        in_specs=(P(row_axes, None), P(row_axes), P(None, row_axes, None, None), P(), P(), P(), P(),
                  P(None, None, 'dp'), P(None, None, 'dp'), P(None, 'dp', None)),
        out_specs=P(row_axes, None),
        check_vma=False,
    )
```
